256 devices in a mesh: dp: 16 (over z, y_lo), mp: 16 (over y_hi, x, core).
Axes of the slice: x: 4, y: 4 (y_hi: 2, y_lo: 2; y = y_hi * 2 + y_lo), z: 8, core: 2. Of those that a mesh axis runs over, the one named last changes fastest.
Arguments:
- gradient: bfloat16 [1, 4096, 4096], P(None, 'mp', 'dp'), may hold values from -6 to 6
- first_moment: float32 [1, 4096, 4096], P(None, 'mp', 'dp'), may hold values from -3 to 3
- second_moment: float32 [1, 4096, 4096], P(None, 'mp', 'dp'), may hold values from 0.0625 to 1
- left_factor: float32 [1, 4096, 4096], P(None, 'mp', 'dp'), may hold values from -18 to 18
- right_factor: float32 [1, 4096, 4096], P(None, 'mp', 'dp'), may hold values from -18 to 18
- left_basis: bfloat16 [1, 4096, 4096], P(None, 'dp', 'mp'), may hold values from -0.09375 to 0.09375
- right_basis: bfloat16 [1, 4096, 4096], P(None, 'mp', 'dp'), may hold values from -0.09375 to 0.09375
Outputs:
- new_first_moment: float32 [1, 4096, 4096], P(None, 'mp', 'dp')
- new_second_moment: float32 [1, 4096, 4096], P(None, 'mp', 'dp')
- new_left_factor: float32 [1, 4096, 4096], P(None, 'mp', 'dp')
- new_right_factor: float32 [1, 4096, 4096], P(None, 'mp', 'dp')
- update: bfloat16 [1, 4096, 4096], P(None, 'mp', 'dp')
The draws below stay inside these ranges and needn't reach their ends.
All inputs are finite; a program needn't handle non-finite values.
Results may differ from the reference program's by a relative error of at most 0.014.
Values may be sent and summed in bfloat16 or wider, within the bound.
No kernel may reach another device: no remote copies, remote signals or barrier semaphores. Data moves between devices by JAX's collectives and lax.ppermute only.
A program may use at most 64 MiB of HBM per device.

```python
import math
import jax
import jax.numpy as jnp
from jax import lax

B = 4096
BLOCKS = 1


def shard_levels(rng, dims, split, low, high):
    def one(position, shards_of):
        steps = jax.random.uniform(jax.random.fold_in(jax.random.fold_in(rng, 6), position), (shards_of,), jnp.float32, low / len(split), high / len(split))
        return jnp.repeat(jnp.exp(steps), dims[position] // shards_of).reshape((-1,) + (1,) * (len(dims) - position - 1))

    level = one(*split[0])
    for cut in split[1:]:
        level = level * one(*cut)
    return level


def scatter_about(stream_key, shape, spread, reach, split=(), dtype=jnp.bfloat16):
    drawn = spread * jax.random.normal(stream_key, shape, jnp.float32)
    if split:
        drawn = drawn * shard_levels(stream_key, shape, split, -0.22, 0.18)
    return jnp.clip(drawn, -reach, reach).astype(dtype)


def setup_inputs(seed: int = 0) -> dict:
    splits = jax.random.split(jax.random.key(seed), 8)
    gradient = scatter_about(splits[0], (BLOCKS, B, B), 1.0, 6.0, ((1, 16), (2, 16)))
    first_moment = scatter_about(splits[1], (BLOCKS, B, B), 0.5, 3.0, ((1, 16), (2, 16)), jnp.float32)
    second_moment = jnp.clip(jnp.exp(math.log(1.0) - 2.7725887 * jax.random.uniform(splits[2], (BLOCKS, B, B), jnp.float32) ** shard_levels(splits[2], (BLOCKS, B, B), ((1, 16), (2, 16)), -0.2, 0.2)), 0.0625, 1.0)
    left_factor = scatter_about(splits[3], (BLOCKS, B, B), 3.0, 18.0, ((1, 16), (2, 16)), jnp.float32)
    right_factor = scatter_about(splits[4], (BLOCKS, B, B), 3.0, 18.0, ((1, 16), (2, 16)), jnp.float32)
    left_basis = scatter_about(splits[5], (BLOCKS, B, B), B ** -0.5, 0.09375, ((1, 16), (2, 16)))
    right_basis = scatter_about(splits[6], (BLOCKS, B, B), B ** -0.5, 0.09375, ((1, 16), (2, 16)))
    return {"gradient": gradient, "first_moment": first_moment, "second_moment": second_moment, "left_factor": left_factor, "right_factor": right_factor, "left_basis": left_basis, "right_basis": right_basis}


decay_moment = 0.95
decay_factor = 0.95
epsilon = 1e-08

def product(left, right):
    return jnp.dot(left.astype(jnp.float32), right.astype(jnp.float32), precision=lax.Precision.HIGHEST)

def single_block(operands):
    gradient, first_moment, second_moment, left_factor, right_factor, left_basis, right_basis = operands
    scale = 1.0 - decay_factor
    new_left = decay_factor * left_factor + scale * product(gradient, gradient.T)
    new_right = decay_factor * right_factor + scale * product(gradient.T, gradient)
    rotated_left = product(left_basis.T, gradient).astype(jnp.bfloat16)
    rotated = product(rotated_left, right_basis)
    new_first = decay_moment * first_moment + (1.0 - decay_moment) * rotated
    new_second = decay_moment * second_moment + (1.0 - decay_moment) * rotated * rotated
    direction = (new_first / (jnp.sqrt(new_second) + epsilon)).astype(jnp.bfloat16)
    back_left = product(left_basis, direction).astype(jnp.bfloat16)
    update = product(back_left, right_basis.T).astype(jnp.bfloat16)
    return (new_first, new_second, new_left, new_right, update)

def reference(gradient, first_moment, second_moment, left_factor, right_factor, left_basis, right_basis):
    first_out, second_out, left_out, right_out, update_out = lax.map(single_block, (gradient, first_moment, second_moment, left_factor, right_factor, left_basis, right_basis))
    return (first_out, second_out, left_out, right_out, update_out)
```

```python
import functools

import jax
import jax.numpy as jnp
from jax import lax
from jax.experimental import pallas as pl
from jax.experimental.pallas import tpu as pltpu
from jax.sharding import PartitionSpec as P

decay_moment = 0.95
decay_factor = 0.95
epsilon = 1e-08


N = 8
SIDE = 256
bf16, f32 = jnp.bfloat16, jnp.float32

TN = (((0,), (0,)), ((), ()))
NN = (((1,), (0,)), ((), ()))
NT = (((1,), (1,)), ((), ()))


def around(i, t):
    return (((i >> 2) + (t >> 2)) & 1) * 4 + ((i + t) & 3)


def back(i, t):
    return (((i >> 2) - (t >> 2)) & 1) * 4 + ((i - t) & 3)


def along_z(x, s):
    return lax.ppermute(x, "dp", [(d, (d + 2 * s) % 16) for d in range(16)])


def along_plane(x, t):
    return lax.ppermute(x, "mp", [(m, 2 * around(m >> 1, t) + (m & 1)) for m in range(16)])


def other_core(x):
    return lax.ppermute(x, "mp", [(m, m ^ 1) for m in range(16)])


def neighbour(x):
    return lax.ppermute(x, "dp", [(d, d ^ 1) for d in range(16)])


def mixed(x, place):
    pairs = []
    for d in range(16):
        for m in range(16):
            y, c = place(d & 1, m & 1)
            pairs.append((((d & ~1) | y) * 16 + ((m & ~1) | c), d * 16 + m))
    return lax.ppermute(x, ("dp", "mp"), pairs)


def swapped(x):
    return mixed(x, lambda y, c: (c, y))


def gather_z(x):
    return [x] + [along_z(x, s) for s in range(1, N)]


def gather_plane(x):
    return [x] + [along_plane(x, t) for t in range(1, N)]


def dot(a, b, dims):
    return lax.dot_general(a, b, dims, preferred_element_type=f32)


def z_back(at, s):
    return (at[0] - s) & 7


def z_on(at, s):
    return (at[0] + s) & 7


def plane_back(at, t):
    return back(at[1], t)


def plane_on(at, t):
    return around(at[1], t)


BLOCK = jax.ShapeDtypeStruct((SIDE, SIDE), bf16)
WIDE = jax.ShapeDtypeStruct((SIDE, SIDE), f32)
PANEL = jax.ShapeDtypeStruct((N, SIDE, SIDE), bf16)


def call(body, at, operands, outs, scratch=(), products=0, name=None):
    vmem = pl.BlockSpec(memory_space=pltpu.VMEM)
    moved = sum(o.size * o.dtype.itemsize for o in (*operands, *outs))
    return pl.pallas_call(
        body,
        out_shape=outs,
        in_specs=[pl.BlockSpec(memory_space=pltpu.SMEM)] + [vmem] * len(operands),
        out_specs=[vmem] * len(outs),
        scratch_shapes=list(scratch),
        cost_estimate=pl.CostEstimate(
            flops=products * 2 * SIDE**3, bytes_accessed=moved, transcendentals=0
        ),
        name=name,
    )(at, *operands)


def pack(at, blocks, place, name):
    def body(at, *refs):
        out = refs[N]
        for s in range(N):
            out[place(at, s)] = refs[s][...]

    return call(body, at, blocks, [PANEL], name=name)[0]


def contract(at, blocks, own, other, dims, keep_panel, name):
    def body(at, *refs):
        parts, (own, other), rest = refs[:N], refs[N : N + 2], refs[N + 2 :]
        keep, send = rest[:2]
        panel = rest[2]
        one, two = rest[3:]
        for s in range(N):
            panel[z_back(at, s)] = parts[s][...]
        one[...] = jnp.zeros_like(one)
        two[...] = jnp.zeros_like(two)

        @pl.loop(0, N)
        def _(j):
            left = panel[j]
            one[...] += dot(left, own[j], dims)
            two[...] += dot(left, other[j], dims)

        mine = at[2] == at[3]

        @pl.when(mine)
        def _():
            keep[...] = one[...]
            send[...] = two[...].astype(bf16)

        @pl.when(jnp.logical_not(mine))
        def _():
            keep[...] = two[...]
            send[...] = one[...].astype(bf16)

    outs = [WIDE, BLOCK] + ([PANEL] if keep_panel else [])
    scratch = [] if keep_panel else [pltpu.VMEM((N, SIDE, SIDE), bf16)]
    scratch += [pltpu.VMEM((SIDE, SIDE), f32)] * 2
    return call(body, at, [*blocks, own, other], outs, scratch, 2 * N, name)


def spread(at, mine, beside, own, other, place, name):
    def body(at, mine, beside, own, other, keep, *rest):
        sends, held = rest[: N - 1], rest[N - 1]
        same = at[2] == at[3]
        one = jnp.where(same, mine[...], beside[...])
        two = jnp.where(same, beside[...], mine[...])

        @pl.loop(0, N)
        def _(j):
            held[j] = dot(one, own[j], NT) + dot(two, other[j], NT)

        keep[...] = held[place(at, 0)]
        for s in range(1, N):
            sends[s - 1][...] = held[place(at, s)].astype(bf16)

    outs = [WIDE] + [BLOCK] * (N - 1)
    scratch = [pltpu.VMEM((N, SIDE, SIDE), f32)]
    return call(body, at, [mine, beside, own, other], outs, scratch, 2 * N, name)


def rotate_back(at, first, second, mine, beside, name):
    def body(at, first, second, mine, beside, keep, *rest):
        sends, held = rest[: N - 1], rest[N - 1]
        same = at[2] == at[3]
        one = jnp.where(same, mine[...], beside[...])
        two = jnp.where(same, beside[...], mine[...])

        @pl.loop(0, N)
        def _(j):
            held[j] = dot(first[j], one, NN) + dot(second[j], two, NN)

        keep[...] = held[plane_on(at, 0)]
        for s in range(1, N):
            sends[s - 1][...] = held[plane_on(at, s)].astype(bf16)

    outs = [WIDE] + [BLOCK] * (N - 1)
    scratch = [pltpu.VMEM((N, SIDE, SIDE), f32)]
    return call(body, at, [first, second, mine, beside], outs, scratch, 2 * N, name)


def right_terms(at, blocks, mine, beside, name):
    def body(at, *refs):
        parts, (mine, beside), rest = refs[:N], refs[N : N + 2], refs[N + 2 :]
        keep, send, panel = rest
        same = at[2] == at[3]
        one = jnp.where(same, mine[...], beside[...])
        two = jnp.where(same, beside[...], mine[...])
        for s in range(N):
            panel[z_back(at, s)] = parts[s][...]

        @pl.loop(0, N)
        def _(j):
            keep[j] = dot(panel[j], one, TN).astype(bf16)
            send[j] = dot(panel[j], two, TN).astype(bf16)

    scratch = [pltpu.VMEM((N, SIDE, SIDE), bf16)]
    return call(body, at, [*blocks, mine, beside], [PANEL, PANEL], scratch, 2 * N, name)


def chip_sum(at, mine, arrived, name):
    def body(at, mine, arrived, keep, *sends):
        def total(s):
            j = plane_on(at, s)
            return mine[j].astype(f32) + arrived[j].astype(f32)

        keep[...] = total(0)
        for s in range(1, N):
            sends[s - 1][...] = total(s).astype(bf16)

    return call(body, at, [mine, arrived], [WIDE] + [BLOCK] * (N - 1), name=name)


def summed(keep, arrived):
    total = keep
    for a in arrived:
        total = total + a.astype(f32)
    return total


def per_device(
    gradient, first_moment, second_moment, left_factor, right_factor, left_basis, right_basis
):
    scale = 1.0 - decay_factor
    g, left, right = gradient[0], left_basis[0], right_basis[0]
    d, m = lax.axis_index("dp"), lax.axis_index("mp")
    at = jnp.stack([d >> 1, m >> 1, m & 1, d & 1]).astype(jnp.int32)

    lefts = gather_z(left)
    g_own = pack(at, gather_plane(swapped(g)), plane_back, "pack_g")
    g_other = other_core(g_own)
    keep, send, left_panel = contract(at, lefts, g_own, g_other, TN, True, "rotate_left")
    rotated_left = (keep + neighbour(send).astype(f32)).astype(bf16)

    r_own = pack(at, gather_plane(swapped(right)), plane_back, "pack_r")
    r_other = other_core(r_own)
    keep, send = contract(at, gather_z(rotated_left), r_own, r_other, NN, False, "rotate_right")
    rotated = keep + neighbour(send).astype(f32)

    new_first = decay_moment * first_moment[0] + (1.0 - decay_moment) * rotated
    new_second = decay_moment * second_moment[0] + (1.0 - decay_moment) * rotated * rotated
    direction = (new_first / (jnp.sqrt(new_second) + epsilon)).astype(bf16)

    first = mixed(left_panel, lambda y, c: (c, y))
    second = mixed(left_panel, lambda y, c: (c, 1 - y))
    keep, *sends = rotate_back(at, first, second, direction, other_core(direction), "back_left")
    back_left = summed(keep, [along_plane(b, t + 1) for t, b in enumerate(sends)]).astype(bf16)
    keep, *sends = spread(at, back_left, neighbour(back_left), r_own, r_other, z_on, "back_right")
    update = summed(keep, [along_z(b, s + 1) for s, b in enumerate(sends)]).astype(bf16)

    g_beside = neighbour(g)
    keep, *sends = spread(at, g, g_beside, g_own, g_other, z_on, "left_factor")
    left_sum = summed(keep, [along_z(b, s + 1) for s, b in enumerate(sends)])
    new_left = decay_factor * left_factor[0] + scale * left_sum

    mine, theirs = right_terms(at, gather_z(g), g, g_beside, "right_terms")
    keep, *sends = chip_sum(at, mine, other_core(theirs), "right_sum")
    right_sum = summed(keep, [along_plane(b, t + 1) for t, b in enumerate(sends)]).astype(bf16)
    new_right = decay_factor * right_factor[0] + scale * swapped(right_sum).astype(f32)
    return tuple(x[None] for x in (new_first, new_second, new_left, new_right, update))


def solution(mesh):
    in_specs = (P(None, "mp", "dp"),) * 5 + (P(None, "dp", "mp"), P(None, "mp", "dp"))
    out_specs = (P(None, "mp", "dp"),) * 5
    return jax.shard_map(
        per_device, mesh=mesh, in_specs=in_specs, out_specs=out_specs, check_vma=False
    )
```

```python
import functools

import jax
import jax.numpy as jnp
from jax import lax
from jax.experimental import pallas as pl
from jax.experimental.pallas import tpu as pltpu
from jax.sharding import PartitionSpec as P

decay_moment = 0.95
decay_factor = 0.95
epsilon = 1e-08


N = 8
SIDE = 256
bf16, f32 = jnp.bfloat16, jnp.float32

TN = (((0,), (0,)), ((), ()))
NN = (((1,), (0,)), ((), ()))
NT = (((1,), (1,)), ((), ()))


def around(i, t):
    return (((i >> 2) + (t >> 2)) & 1) * 4 + ((i + t) & 3)


def back(i, t):
    return (((i >> 2) - (t >> 2)) & 1) * 4 + ((i - t) & 3)


def along_z(x, s):
    return lax.ppermute(x, "dp", [(d, (d + 2 * s) % 16) for d in range(16)])


def along_plane(x, t):
    return lax.ppermute(x, "mp", [(m, 2 * around(m >> 1, t) + (m & 1)) for m in range(16)])


def other_core(x):
    return lax.ppermute(x, "mp", [(m, m ^ 1) for m in range(16)])


def neighbour(x):
    return lax.ppermute(x, "dp", [(d, d ^ 1) for d in range(16)])


def mixed(x, place):
    pairs = []
    for d in range(16):
        for m in range(16):
            y, c = place(d & 1, m & 1)
            pairs.append((((d & ~1) | y) * 16 + ((m & ~1) | c), d * 16 + m))
    return lax.ppermute(x, ("dp", "mp"), pairs)


def to_swapped(x, t):
    pairs = []
    for d in range(16):
        for m in range(16):
            to_d = (d & ~1) | (m & 1)
            to_m = 2 * around(m >> 1, t) + (d & 1)
            pairs.append((d * 16 + m, to_d * 16 + to_m))
    return lax.ppermute(x, ("dp", "mp"), pairs)


Z_GROUPS = [[2 * z + y for z in range(N)] for y in range(2)]
PLANE_GROUPS = [[2 * i + c for i in range(N)] for c in range(2)]


def exchange(x, axis, groups):
    return lax.all_to_all(x, axis, 0, 0, axis_index_groups=groups, tiled=True)


def exchange_z(x):
    return exchange(x, "dp", Z_GROUPS)


def exchange_plane(x):
    return exchange(x, "mp", PLANE_GROUPS)


def everywhere_z(x):
    return exchange_z(jnp.broadcast_to(x, (N, *x.shape)))


def gather_z(x):
    return [x] + [along_z(x, s) for s in range(1, N)]


def dot(a, b, dims):
    return lax.dot_general(a, b, dims, preferred_element_type=f32)


def z_back(at, s):
    return (at[0] - s) & 7


def z_on(at, s):
    return (at[0] + s) & 7


def plane_back(at, t):
    return back(at[1], t)


def plane_on(at, t):
    return around(at[1], t)


BLOCK = jax.ShapeDtypeStruct((SIDE, SIDE), bf16)
WIDE = jax.ShapeDtypeStruct((SIDE, SIDE), f32)
PANEL = jax.ShapeDtypeStruct((N, SIDE, SIDE), bf16)


def call(body, at, operands, outs, scratch=(), products=0, name=None):
    vmem = pl.BlockSpec(memory_space=pltpu.VMEM)
    moved = sum(o.size * o.dtype.itemsize for o in (*operands, *outs))
    return pl.pallas_call(
        body,
        out_shape=outs,
        in_specs=[pl.BlockSpec(memory_space=pltpu.SMEM)] + [vmem] * len(operands),
        out_specs=[vmem] * len(outs),
        scratch_shapes=list(scratch),
        cost_estimate=pl.CostEstimate(
            flops=products * 2 * SIDE**3, bytes_accessed=moved, transcendentals=0
        ),
        name=name,
    )(at, *operands)


def pack(at, pairs, name):
    def body(at, *refs):
        one, two = refs[N:]
        for t in range(N):
            j = plane_back(at, t)
            one[j] = refs[t][0]
            two[j] = refs[t][1]

    return call(body, at, pairs, [PANEL, PANEL], name=name)


def contract(at, blocks, own, other, dims, name):
    def body(at, blocks, own, other, keep, send):
        if dims == TN:
            left = blocks[...].reshape(N * SIDE, SIDE)
        else:
            left = jnp.concatenate([blocks[j] for j in range(N)], axis=1)
        one = dot(left, own[...].reshape(N * SIDE, SIDE), dims)
        two = dot(left, other[...].reshape(N * SIDE, SIDE), dims)
        same = at[2] == at[3]
        keep[...] = jnp.where(same, one, two)
        send[...] = jnp.where(same, two, one).astype(bf16)

    return call(body, at, [blocks, own, other], [WIDE, BLOCK], (), 2 * N, name)


def ordered(at, mine, beside, axis):
    same = at[2] == at[3]
    one = jnp.where(same, mine[...], beside[...])
    two = jnp.where(same, beside[...], mine[...])
    return jnp.concatenate([one, two], axis=axis)


def spread(at, mine, beside, own, other, name, apart=False):
    def body(at, mine, beside, own, other, *rest):
        both = ordered(at, mine, beside, 1)
        held = rest[-1]

        @pl.loop(0, N)
        def _(j):
            right = jnp.concatenate([own[j], other[j]], axis=1)
            held[j] = dot(both, right, NT).astype(held.dtype)

        if apart:
            rest[0][...] = held[z_on(at, 0)]
            for s in range(1, N):
                rest[s][...] = held[z_on(at, s)].astype(bf16)

    outs = [WIDE] + [BLOCK] * (N - 1) if apart else [PANEL]
    scratch = [pltpu.VMEM((N, SIDE, SIDE), f32)] if apart else []
    return call(body, at, [mine, beside, own, other], outs, scratch, 2 * N, name)


def rotate_back(at, first, second, mine, beside, name):
    def body(at, first, second, mine, beside, out):
        both = ordered(at, mine, beside, 0)

        @pl.loop(0, N)
        def _(j):
            left = jnp.concatenate([first[j], second[j]], axis=1)
            out[j] = dot(left, both, NN).astype(bf16)

    return call(body, at, [first, second, mine, beside], [PANEL], (), 2 * N, name)[0]


def right_terms(at, blocks, mine, beside, name):
    def body(at, *refs):
        parts, (mine, beside), rest = refs[:N], refs[N : N + 2], refs[N + 2 :]
        keep, send, panel = rest
        both = ordered(at, mine, beside, 1)
        for s in range(N):
            panel[z_back(at, s)] = parts[s][...]

        @pl.loop(0, N)
        def _(j):
            term = dot(panel[j], both, TN).astype(bf16)
            keep[j] = term[:, :SIDE]
            send[j] = term[:, SIDE:]

    scratch = [pltpu.VMEM((N, SIDE, SIDE), bf16)]
    return call(body, at, [*blocks, mine, beside], [PANEL, PANEL], scratch, 2 * N, name)


def chip_sum(at, mine, arrived, name):
    def body(at, mine, arrived, *sends):
        for t in range(N):
            j = plane_on(at, t)
            sends[t][...] = (mine[j].astype(f32) + arrived[j].astype(f32)).astype(bf16)

    return call(body, at, [mine, arrived], [BLOCK] * N, name=name)


def summed(keep, arrived):
    total = keep
    for a in arrived:
        total = total + a.astype(f32)
    return total


def per_device(
    gradient, first_moment, second_moment, left_factor, right_factor, left_basis, right_basis
):
    scale = 1.0 - decay_factor
    g, left, right = gradient[0], left_basis[0], right_basis[0]
    d, m = lax.axis_index("dp"), lax.axis_index("mp")
    at = jnp.stack([d >> 1, m >> 1, m & 1, d & 1]).astype(jnp.int32)

    left_panel = everywhere_z(left)
    both = jnp.stack([g, right])
    g_own, r_own = pack(at, [to_swapped(both, t) for t in range(N)], "pack")
    g_other, r_other = other_core(g_own), other_core(r_own)
    g_beside = neighbour(g)

    keep, send = contract(at, left_panel, g_own, g_other, TN, "rotate_left")
    rotated_left = everywhere_z((keep + neighbour(send).astype(f32)).astype(bf16))
    keep, send = contract(at, rotated_left, r_own, r_other, NN, "rotate_right")
    rotated = keep + neighbour(send).astype(f32)

    new_first = decay_moment * first_moment[0] + (1.0 - decay_moment) * rotated
    new_second = decay_moment * second_moment[0] + (1.0 - decay_moment) * rotated * rotated
    direction = (new_first / (jnp.sqrt(new_second) + epsilon)).astype(bf16)

    first = mixed(left_panel, lambda y, c: (c, y))
    second = mixed(left_panel, lambda y, c: (c, 1 - y))
    terms = rotate_back(at, first, second, direction, other_core(direction), "back_left")
    back_left = jnp.sum(exchange_plane(terms), axis=0, dtype=f32).astype(bf16)
    terms = spread(at, back_left, neighbour(back_left), r_own, r_other, "back_right")[0]
    update = jnp.sum(exchange_z(terms), axis=0, dtype=f32).astype(bf16)

    keep, *sends = spread(at, g, g_beside, g_own, g_other, "left_factor", True)
    left_sum = summed(keep, [along_z(b, s + 1) for s, b in enumerate(sends)])
    new_left = decay_factor * left_factor[0] + scale * left_sum

    mine, theirs = right_terms(at, gather_z(g), g, g_beside, "right_terms")
    sends = chip_sum(at, mine, other_core(theirs), "right_sum")
    right_sum = summed(0.0, [to_swapped(b, t) for t, b in enumerate(sends)])
    new_right = decay_factor * right_factor[0] + scale * right_sum
    return tuple(x[None] for x in (new_first, new_second, new_left, new_right, update))


def solution(mesh):
    in_specs = (P(None, "mp", "dp"),) * 5 + (P(None, "dp", "mp"), P(None, "mp", "dp"))
    out_specs = (P(None, "mp", "dp"),) * 5
    return jax.shard_map(
        per_device, mesh=mesh, in_specs=in_specs, out_specs=out_specs, check_vma=False
    )
```

```python
import jax
import jax.numpy as jnp
from jax import lax
from jax.experimental import pallas as pl
from jax.experimental.pallas import tpu as pltpu
from jax.sharding import PartitionSpec as P


decay_moment = 0.95
decay_factor = 0.95
epsilon = 1e-08


N = 8
SIDE = 256
bf16, f32 = jnp.bfloat16, jnp.float32

TN = (((0,), (0,)), ((), ()))
NN = (((1,), (0,)), ((), ()))
NT = (((1,), (1,)), ((), ()))


def around(i, t):
    return (((i >> 2) + (t >> 2)) & 1) * 4 + ((i + t) & 3)


def back(i, t):
    return (((i >> 2) - (t >> 2)) & 1) * 4 + ((i - t) & 3)


def along_z(x, s):
    return lax.ppermute(x, "dp", [(d, (d + 2 * s) % 16) for d in range(16)])


def other_core(x):
    return lax.ppermute(x, "mp", [(m, m ^ 1) for m in range(16)])


def neighbour(x):
    return lax.ppermute(x, "dp", [(d, d ^ 1) for d in range(16)])


def mixed(x, place):
    pairs = []
    for d in range(16):
        for m in range(16):
            y, c = place(d & 1, m & 1)
            pairs.append((((d & ~1) | y) * 16 + ((m & ~1) | c), d * 16 + m))
    return lax.ppermute(x, ("dp", "mp"), pairs)


def to_swapped(x, t):
    pairs = []
    for d in range(16):
        for m in range(16):
            to_d = (d & ~1) | (m & 1)
            to_m = 2 * around(m >> 1, t) + (d & 1)
            pairs.append((d * 16 + m, to_d * 16 + to_m))
    return lax.ppermute(x, ("dp", "mp"), pairs)


Z_GROUPS = [[2 * z + y for z in range(N)] for y in range(2)]
PLANE_GROUPS = [[2 * i + c for i in range(N)] for c in range(2)]


def exchange(x, axis, groups):
    return lax.all_to_all(x, axis, 0, 0, axis_index_groups=groups, tiled=True)


def exchange_z(x):
    return exchange(x, "dp", Z_GROUPS)


def exchange_plane(x):
    return exchange(x, "mp", PLANE_GROUPS)


def everywhere_z(x):
    return exchange_z(jnp.broadcast_to(x, (N, *x.shape)))


def gather_z(x):
    return [x] + [along_z(x, s) for s in range(1, N)]


def dot(a, b, dims):
    return lax.dot_general(a, b, dims, preferred_element_type=f32)


def z_back(at, s):
    return (at[0] - s) & 7


def z_on(at, s):
    return (at[0] + s) & 7


def plane_back(at, t):
    return back(at[1], t)


def plane_on(at, t):
    return around(at[1], t)


BLOCK = jax.ShapeDtypeStruct((SIDE, SIDE), bf16)
WIDE = jax.ShapeDtypeStruct((SIDE, SIDE), f32)
PANEL = jax.ShapeDtypeStruct((N, SIDE, SIDE), bf16)


def call(body, at, operands, outs, scratch=(), products=0):
    vmem = pl.BlockSpec(memory_space=pltpu.VMEM)
    moved = sum(o.size * o.dtype.itemsize for o in (*operands, *outs))
    return pl.pallas_call(
        body,
        out_shape=outs,
        in_specs=[pl.BlockSpec(memory_space=pltpu.SMEM)] + [vmem] * len(operands),
        out_specs=[vmem] * len(outs),
        scratch_shapes=list(scratch),
        cost_estimate=pl.CostEstimate(
            flops=products * 2 * SIDE**3, bytes_accessed=moved, transcendentals=0
        ),
    )(at, *operands)


def pack(at, blocks):
    def body(at, *refs):
        for t in range(N):
            refs[N][plane_back(at, t)] = refs[t][...]

    return call(body, at, blocks, [PANEL])[0]


def contract(at, blocks, own, other, dims):
    def body(at, blocks, own, other, keep, send):
        if dims == TN:
            left = blocks[...].reshape(N * SIDE, SIDE)
        else:
            left = jnp.concatenate([blocks[j] for j in range(N)], axis=1)
        one = dot(left, own[...].reshape(N * SIDE, SIDE), dims)
        two = dot(left, other[...].reshape(N * SIDE, SIDE), dims)
        same = at[2] == at[3]
        keep[...] = jnp.where(same, one, two)
        send[...] = jnp.where(same, two, one).astype(bf16)

    return call(body, at, [blocks, own, other], [WIDE, BLOCK], (), 2 * N)


def ordered(at, mine, beside, axis):
    same = at[2] == at[3]
    one = jnp.where(same, mine[...], beside[...])
    two = jnp.where(same, beside[...], mine[...])
    return jnp.concatenate([one, two], axis=axis)


def spread(at, mine, beside, own, other, apart=False):
    def body(at, mine, beside, own, other, *rest):
        both = ordered(at, mine, beside, 1)
        held = rest[-1]

        @pl.loop(0, N, step=2)
        def _(j):
            two = pl.ds(j, 2)
            right = jnp.concatenate(
                [own[two].reshape(2 * SIDE, SIDE), other[two].reshape(2 * SIDE, SIDE)], axis=1
            )
            pair = dot(both, right, NT).astype(held.dtype)
            held[j] = pair[:, :SIDE]
            held[j + 1] = pair[:, SIDE:]

        if apart:
            rest[0][...] = held[z_on(at, 0)]
            for s in range(1, N):
                rest[s][...] = held[z_on(at, s)].astype(bf16)

    outs = [WIDE] + [BLOCK] * (N - 1) if apart else [PANEL]
    scratch = [pltpu.VMEM((N, SIDE, SIDE), f32)] if apart else []
    return call(body, at, [mine, beside, own, other], outs, scratch, 2 * N)


def rotate_back(at, first, second, mine, beside):
    def body(at, first, second, mine, beside, out):
        both = ordered(at, mine, beside, 0)

        @pl.loop(0, N, step=2)
        def _(j):
            two = pl.ds(j, 2)
            left = jnp.concatenate(
                [first[two].reshape(2 * SIDE, SIDE), second[two].reshape(2 * SIDE, SIDE)], axis=1
            )
            out[two] = dot(left, both, NN).astype(bf16).reshape(2, SIDE, SIDE)

    return call(body, at, [first, second, mine, beside], [PANEL], (), 2 * N)[0]


def right_terms(at, blocks, mine, beside):
    def body(at, *refs):
        parts, (mine, beside), rest = refs[:N], refs[N : N + 2], refs[N + 2 :]
        keep, send, panel = rest
        both = ordered(at, mine, beside, 1)
        for s in range(N):
            panel[z_back(at, s)] = parts[s][...]

        @pl.loop(0, N)
        def _(j):
            term = dot(panel[j], both, TN).astype(bf16)
            keep[j] = term[:, :SIDE]
            send[j] = term[:, SIDE:]

    scratch = [pltpu.VMEM((N, SIDE, SIDE), bf16)]
    return call(body, at, [*blocks, mine, beside], [PANEL, PANEL], scratch, 2 * N)


def chip_sum(at, mine, arrived):
    def body(at, mine, arrived, *sends):
        for t in range(N):
            j = plane_on(at, t)
            sends[t][...] = (mine[j].astype(f32) + arrived[j].astype(f32)).astype(bf16)

    return call(body, at, [mine, arrived], [BLOCK] * N)


def summed(keep, arrived):
    total = keep
    for a in arrived:
        total = total + a.astype(f32)
    return total


def update_step(
    gradient, first_moment, second_moment, left_factor, right_factor, left_basis, right_basis
):
    scale = 1.0 - decay_factor
    g, left, right = gradient[0], left_basis[0], right_basis[0]
    d, m = lax.axis_index("dp"), lax.axis_index("mp")
    at = jnp.stack([d >> 1, m >> 1, m & 1, d & 1]).astype(jnp.int32)

    left_panel = everywhere_z(left)
    arrived = [to_swapped(g, t) for t in range(N)]
    g_own = pack(at, arrived)
    r_block = to_swapped(right, 0)
    r_own = exchange_plane(jnp.broadcast_to(r_block, (N, SIDE, SIDE)))
    g_other = other_core(g_own)
    r_other = other_core(r_own)
    g_beside = neighbour(g)

    keep, send = contract(at, left_panel, g_own, g_other, TN)
    turned = neighbour(send)
    rotated_left = (keep + turned.astype(f32)).astype(bf16)
    rotated_left = everywhere_z(rotated_left)
    keep, send = contract(at, rotated_left, r_own, r_other, NN)
    turned = neighbour(send)
    rotated = keep + turned.astype(f32)

    new_first = decay_moment * first_moment[0] + (1.0 - decay_moment) * rotated
    new_second = decay_moment * second_moment[0] + (1.0 - decay_moment) * rotated * rotated
    direction = (new_first / (jnp.sqrt(new_second) + epsilon)).astype(bf16)

    first = mixed(left_panel, lambda y, c: (c, y))
    second = mixed(left_panel, lambda y, c: (c, 1 - y))
    direction_beside = other_core(direction)
    terms = rotate_back(at, first, second, direction, direction_beside)
    terms = exchange_plane(terms)
    back_left = jnp.sum(terms, axis=0, dtype=f32).astype(bf16)
    back_beside = neighbour(back_left)
    terms = spread(at, back_left, back_beside, r_own, r_other)[0]
    terms = exchange_z(terms)
    update = jnp.sum(terms, axis=0, dtype=f32).astype(bf16)

    keep, *sends = spread(at, g, g_beside, g_own, g_other, True)
    arrived = [along_z(b, s + 1) for s, b in enumerate(sends)]
    new_left = decay_factor * left_factor[0] + scale * summed(keep, arrived)

    row = gather_z(g)
    mine, theirs = right_terms(at, row, g, g_beside)
    theirs = other_core(theirs)
    sends = chip_sum(at, mine, theirs)
    arrived = [to_swapped(b, t) for t, b in enumerate(sends)]
    new_right = decay_factor * right_factor[0] + scale * summed(0.0, arrived)
    return tuple(x[None] for x in (new_first, new_second, new_left, new_right, update))


def solution(mesh):
    in_specs = (P(None, "mp", "dp"),) * 5 + (P(None, "dp", "mp"), P(None, "mp", "dp"))
    out_specs = (P(None, "mp", "dp"),) * 5
    return jax.shard_map(
        update_step, mesh=mesh, in_specs=in_specs, out_specs=out_specs, check_vma=False
    )
```

```python
import jax
import jax.numpy as jnp
from jax import lax
from jax.experimental import pallas as pl
from jax.experimental.pallas import tpu as pltpu
from jax.sharding import PartitionSpec as P


decay_moment = 0.95
decay_factor = 0.95
epsilon = 1e-08


N = 8
SIDE = 256
bf16, f32 = jnp.bfloat16, jnp.float32

TN = (((0,), (0,)), ((), ()))
NN = (((1,), (0,)), ((), ()))
NT = (((1,), (1,)), ((), ()))


def around(i, t):
    return (((i >> 2) + (t >> 2)) & 1) * 4 + ((i + t) & 3)


def back(i, t):
    return (((i >> 2) - (t >> 2)) & 1) * 4 + ((i - t) & 3)


def other_core(x):
    return lax.ppermute(x, "mp", [(m, m ^ 1) for m in range(16)])


def neighbour(x):
    return lax.ppermute(x, "dp", [(d, d ^ 1) for d in range(16)])


def placed(x, to):
    pairs = []
    for d in range(16):
        for m in range(16):
            to_d, to_m = to(d, m)
            pairs.append((d * 16 + m, to_d * 16 + to_m))
    return lax.ppermute(x, ("dp", "mp"), pairs)


def swap(d, m):
    return (d & ~1) | (m & 1), (m & ~1) | (d & 1)


def to_swapped(x, t):
    return placed(x, lambda d, m: swap(d, 2 * around(m >> 1, t) + (m & 1)))


Z_GROUPS = [[2 * z + y for z in range(N)] for y in range(2)]
PLANE_GROUPS = [[2 * i + c for i in range(N)] for c in range(2)]


def exchange(x, axis, groups):
    return lax.all_to_all(x, axis, 0, 0, axis_index_groups=groups, tiled=True)


def exchange_z(x):
    return exchange(x, "dp", Z_GROUPS)


def exchange_plane(x):
    return exchange(x, "mp", PLANE_GROUPS)


def everywhere_z(x):
    return exchange_z(jnp.broadcast_to(x, (N, *x.shape)))


def from_plane(x):
    arrived = {t: to_swapped(x, t) for t in (6, 5, 7, 2, 4, 1, 3, 0)}
    return [arrived[t] for t in range(N)]


def dot(a, b, dims):
    return lax.dot_general(a, b, dims, preferred_element_type=f32)


def plane_back(at, t):
    return back(at[1], t)


def plane_on(at, t):
    return around(at[1], t)


BLOCK = jax.ShapeDtypeStruct((SIDE, SIDE), bf16)
WIDE = jax.ShapeDtypeStruct((SIDE, SIDE), f32)
PANEL = jax.ShapeDtypeStruct((N, SIDE, SIDE), bf16)


def call(body, at, operands, outs, scratch=(), products=0, part=None):
    vmem = pl.BlockSpec(memory_space=pltpu.VMEM)
    first = vmem
    if part is not None:
        first = pl.BlockSpec((None, N, SIDE, SIDE), lambda _: (part, 0, 0, 0))
    moved = sum(o.size * o.dtype.itemsize for o in (*operands, *outs))
    return pl.pallas_call(
        body,
        out_shape=outs,
        grid=() if part is None else (1,),
        in_specs=[pl.BlockSpec(memory_space=pltpu.SMEM), first] + [vmem] * (len(operands) - 1),
        out_specs=[vmem] * len(outs),
        scratch_shapes=list(scratch),
        cost_estimate=pl.CostEstimate(
            flops=products * 2 * SIDE**3, bytes_accessed=moved, transcendentals=0
        ),
    )(at, *operands)


def pack(at, blocks):
    def body(at, *refs):
        for t in range(N):
            refs[N][plane_back(at, t)] = refs[t][...]

    return call(body, at, blocks, [PANEL])[0]


def contract(at, blocks, own, other, dims, part=None):
    def body(at, blocks, own, other, keep, send):
        if dims == TN:
            left = blocks[...].reshape(N * SIDE, SIDE)
        else:
            left = jnp.concatenate([blocks[j] for j in range(N)], axis=1)
        one = dot(left, own[...].reshape(N * SIDE, SIDE), dims)
        two = dot(left, other[...].reshape(N * SIDE, SIDE), dims)
        same = at[2] == at[3]
        keep[...] = jnp.where(same, one, two)
        send[...] = jnp.where(same, two, one).astype(bf16)

    return call(body, at, [blocks, own, other], [WIDE, BLOCK], (), 2 * N, part)


def ordered(at, mine, beside, axis):
    same = at[2] == at[3]
    one = jnp.where(same, mine[...], beside[...])
    two = jnp.where(same, beside[...], mine[...])
    return jnp.concatenate([one, two], axis=axis)


def spread(at, mine, beside, own, other):
    def body(at, mine, beside, own, other, out):
        both = ordered(at, mine, beside, 1)

        @pl.loop(0, N, step=2)
        def _(j):
            two = pl.ds(j, 2)
            right = jnp.concatenate(
                [own[two].reshape(2 * SIDE, SIDE), other[two].reshape(2 * SIDE, SIDE)], axis=1
            )
            pair = dot(both, right, NT).astype(bf16)
            out[j] = pair[:, :SIDE]
            out[j + 1] = pair[:, SIDE:]

    return call(body, at, [mine, beside, own, other], [PANEL], (), 2 * N)[0]


def rotate_back(at, first, second, mine, beside):
    def body(at, first, second, mine, beside, out):
        both = ordered(at, mine, beside, 0)

        @pl.loop(0, N, step=2)
        def _(j):
            two = pl.ds(j, 2)
            left = jnp.concatenate(
                [first[two].reshape(2 * SIDE, SIDE), second[two].reshape(2 * SIDE, SIDE)], axis=1
            )
            out[two] = dot(left, both, NN).astype(bf16).reshape(2, SIDE, SIDE)

    return call(body, at, [first, second, mine, beside], [PANEL], (), 2 * N)[0]


def right_terms(at, row, mine, beside):
    def body(at, row, mine, beside, keep, send):
        both = ordered(at, mine, beside, 1)

        @pl.loop(0, N)
        def _(j):
            term = dot(row[j], both, TN).astype(bf16)
            keep[j] = term[:, :SIDE]
            send[j] = term[:, SIDE:]

    return call(body, at, [row, mine, beside], [PANEL, PANEL], (), 2 * N, 1)


def chip_sum(at, mine, arrived):
    def body(at, mine, arrived, *sends):
        for t in range(N):
            j = plane_on(at, t)
            sends[t][...] = (mine[j].astype(f32) + arrived[j].astype(f32)).astype(bf16)

    return call(body, at, [mine, arrived], [BLOCK] * N)


def update_step(
    gradient, first_moment, second_moment, left_factor, right_factor, left_basis, right_basis
):
    scale = 1.0 - decay_factor
    g, left, right = gradient[0], left_basis[0], right_basis[0]
    d, m = lax.axis_index("dp"), lax.axis_index("mp")
    at = jnp.stack([d >> 1, m >> 1, m & 1, d & 1]).astype(jnp.int32)

    both = lax.all_gather(
        jnp.stack([left, g]), "dp", axis=1, axis_index_groups=Z_GROUPS, tiled=True
    )
    both = both.reshape(2, N, SIDE, SIDE)
    r_block = to_swapped(right, 0)
    g_own = from_plane(g)
    g_own = pack(at, g_own)
    r_own = exchange_plane(jnp.broadcast_to(r_block, (N, SIDE, SIDE)))
    g_other = other_core(g_own)
    r_other = other_core(r_own)
    g_beside = neighbour(g)

    keep, send = contract(at, both, g_own, g_other, TN, 0)
    turned = neighbour(send)
    rotated_left = (keep + turned.astype(f32)).astype(bf16)
    rotated_left = everywhere_z(rotated_left)
    keep, send = contract(at, rotated_left, r_own, r_other, NN)
    terms = spread(at, g, g_beside, g_own, g_other)
    terms = lax.optimization_barrier((terms, keep))[0].reshape(N * SIDE, SIDE)
    left_sum = lax.psum_scatter(terms, "dp", axis_index_groups=Z_GROUPS, tiled=True)
    new_left = decay_factor * left_factor[0] + scale * left_sum.astype(f32)
    turned = neighbour(send)
    rotated = keep + turned.astype(f32)

    new_first = decay_moment * first_moment[0] + (1.0 - decay_moment) * rotated
    new_second = decay_moment * second_moment[0] + (1.0 - decay_moment) * rotated * rotated
    direction = (new_first / (jnp.sqrt(new_second) + epsilon)).astype(bf16)

    left_panel = both[0]
    first = placed(left_panel, swap)
    second = placed(left_panel, lambda d, m: swap(d, m ^ 1))
    direction_beside = other_core(direction)
    terms = rotate_back(at, first, second, direction, direction_beside)
    terms = exchange_plane(terms)
    back_left = jnp.sum(terms, axis=0, dtype=f32).astype(bf16)
    back_beside = neighbour(back_left)
    terms = spread(at, back_left, back_beside, r_own, r_other)
    terms = exchange_z(terms)
    update = jnp.sum(terms, axis=0, dtype=f32).astype(bf16)

    mine, theirs = right_terms(at, both, g, g_beside)
    theirs = other_core(theirs)
    sends = chip_sum(at, mine, theirs)
    arrived = [to_swapped(sends[t], t) for t in (6, 5, 7, 2)]
    arrived += [to_swapped(sends[t], t) for t in (4, 1, 3, 0)]
    right_sum = sum(a.astype(f32) for a in arrived)
    new_right = decay_factor * right_factor[0] + scale * right_sum
    return tuple(x[None] for x in (new_first, new_second, new_left, new_right, update))


def solution(mesh):
    in_specs = (P(None, "mp", "dp"),) * 5 + (P(None, "dp", "mp"), P(None, "mp", "dp"))
    out_specs = (P(None, "mp", "dp"),) * 5
    return jax.shard_map(
        update_step, mesh=mesh, in_specs=in_specs, out_specs=out_specs, check_vma=False
    )
```

```python
import jax
import jax.numpy as jnp
from jax import lax
from jax.experimental import pallas as pl
from jax.experimental.pallas import tpu as pltpu
from jax.sharding import PartitionSpec as P


decay_moment = 0.95
decay_factor = 0.95
epsilon = 1e-08


N = 8
SIDE = 256
bf16, f32 = jnp.bfloat16, jnp.float32

TN = (((0,), (0,)), ((), ()))
NN = (((1,), (0,)), ((), ()))
NT = (((1,), (1,)), ((), ()))


def around(i, t):
    return (((i >> 2) + (t >> 2)) & 1) * 4 + ((i + t) & 3)


def back(i, t):
    return (((i >> 2) - (t >> 2)) & 1) * 4 + ((i - t) & 3)


def along_z(x, s):
    return lax.ppermute(x, "dp", [(d, (d + 2 * s) % 16) for d in range(16)])


def other_core(x):
    return lax.ppermute(x, "mp", [(m, m ^ 1) for m in range(16)])


def neighbour(x):
    return lax.ppermute(x, "dp", [(d, d ^ 1) for d in range(16)])


def placed(x, to):
    pairs = []
    for d in range(16):
        for m in range(16):
            to_d, to_m = to(d, m)
            pairs.append((d * 16 + m, to_d * 16 + to_m))
    return lax.ppermute(x, ("dp", "mp"), pairs)


def swap(d, m):
    return (d & ~1) | (m & 1), (m & ~1) | (d & 1)


def to_swapped(x, t):
    return placed(x, lambda d, m: swap(d, 2 * around(m >> 1, t) + (m & 1)))


Z_GROUPS = [[2 * z + y for z in range(N)] for y in range(2)]
PLANE_GROUPS = [[2 * i + c for i in range(N)] for c in range(2)]


def exchange(x, axis, groups):
    return lax.all_to_all(x, axis, 0, 0, axis_index_groups=groups, tiled=True)


def exchange_z(x):
    return exchange(x, "dp", Z_GROUPS)


def exchange_plane(x):
    return exchange(x, "mp", PLANE_GROUPS)


def from_plane(x):
    arrived = {t: to_swapped(x, t) for t in (6, 5, 7, 2, 4, 1, 3, 0)}
    return [arrived[t] for t in range(N)]


def dot(a, b, dims):
    return lax.dot_general(a, b, dims, preferred_element_type=f32)


def z_on(at, s):
    return (at[0] + s) & 7


def plane_back(at, t):
    return back(at[1], t)


def plane_on(at, t):
    return around(at[1], t)


BLOCK = jax.ShapeDtypeStruct((SIDE, SIDE), bf16)
WIDE = jax.ShapeDtypeStruct((SIDE, SIDE), f32)
PANEL = jax.ShapeDtypeStruct((N, SIDE, SIDE), bf16)


def call(body, at, operands, outs, scratch=(), products=0, part=None):
    vmem = pl.BlockSpec(memory_space=pltpu.VMEM)
    first = vmem
    if part is not None:
        first = pl.BlockSpec((None, N, SIDE, SIDE), lambda _: (part, 0, 0, 0))
    moved = sum(o.size * o.dtype.itemsize for o in (*operands, *outs))
    return pl.pallas_call(
        body,
        out_shape=outs,
        grid=() if part is None else (1,),
        in_specs=[pl.BlockSpec(memory_space=pltpu.SMEM), first] + [vmem] * (len(operands) - 1),
        out_specs=[vmem] * len(outs),
        scratch_shapes=list(scratch),
        cost_estimate=pl.CostEstimate(
            flops=products * 2 * SIDE**3, bytes_accessed=moved, transcendentals=0
        ),
    )(at, *operands)


def pack(at, blocks):
    def body(at, *refs):
        for t in range(N):
            refs[N][plane_back(at, t)] = refs[t][...]

    return call(body, at, blocks, [PANEL])[0]


def contract(at, blocks, own, other, dims, part=None):
    def body(at, blocks, own, other, keep, send):
        if dims == TN:
            left = blocks[...].reshape(N * SIDE, SIDE)
        else:
            left = jnp.concatenate([blocks[j] for j in range(N)], axis=1)
        one = dot(left, own[...].reshape(N * SIDE, SIDE), dims)
        two = dot(left, other[...].reshape(N * SIDE, SIDE), dims)
        same = at[2] == at[3]
        keep[...] = jnp.where(same, one, two)
        send[...] = jnp.where(same, two, one).astype(bf16)

    return call(body, at, [blocks, own, other], [WIDE, BLOCK], (), 2 * N, part)


def ordered(at, mine, beside, axis):
    same = at[2] == at[3]
    one = jnp.where(same, mine[...], beside[...])
    two = jnp.where(same, beside[...], mine[...])
    return jnp.concatenate([one, two], axis=axis)


def spread(at, mine, beside, own, other):
    def body(at, mine, beside, own, other, out):
        both = ordered(at, mine, beside, 1)

        @pl.loop(0, N, step=2)
        def _(j):
            two = pl.ds(j, 2)
            right = jnp.concatenate(
                [own[two].reshape(2 * SIDE, SIDE), other[two].reshape(2 * SIDE, SIDE)], axis=1
            )
            pair = dot(both, right, NT).astype(bf16)
            out[j] = pair[:, :SIDE]
            out[j + 1] = pair[:, SIDE:]

    return call(body, at, [mine, beside, own, other], [PANEL], (), 2 * N)[0]


def spread_apart(at, mine, beside, own, other):
    def body(at, mine, beside, own, other, keep, *sends):
        both = ordered(at, mine, beside, 1)
        for s in range(N):
            j = z_on(at, s)
            term = dot(both, jnp.concatenate([own[j], other[j]], axis=1), NT)
            if s == 0:
                keep[...] = term
            else:
                sends[s - 1][...] = term.astype(bf16)

    outs = [WIDE] + [BLOCK] * (N - 1)
    return call(body, at, [mine, beside, own, other], outs, (), 2 * N)


def rotate_back(at, first, second, mine, beside):
    def body(at, first, second, mine, beside, out):
        both = ordered(at, mine, beside, 0)

        @pl.loop(0, N, step=2)
        def _(j):
            two = pl.ds(j, 2)
            left = jnp.concatenate(
                [first[two].reshape(2 * SIDE, SIDE), second[two].reshape(2 * SIDE, SIDE)], axis=1
            )
            out[two] = dot(left, both, NN).astype(bf16).reshape(2, SIDE, SIDE)

    return call(body, at, [first, second, mine, beside], [PANEL], (), 2 * N)[0]


def right_terms(at, row, mine, beside):
    def body(at, row, mine, beside, keep, send):
        both = ordered(at, mine, beside, 1)

        @pl.loop(0, N)
        def _(j):
            term = dot(row[j], both, TN).astype(bf16)
            keep[j] = term[:, :SIDE]
            send[j] = term[:, SIDE:]

    return call(body, at, [row, mine, beside], [PANEL, PANEL], (), 2 * N, 1)


def chip_sum(at, mine, arrived):
    def body(at, mine, arrived, *sends):
        for t in range(N):
            j = plane_on(at, t)
            sends[t][...] = (mine[j].astype(f32) + arrived[j].astype(f32)).astype(bf16)

    return call(body, at, [mine, arrived], [BLOCK] * N)


def update_step(
    gradient, first_moment, second_moment, left_factor, right_factor, left_basis, right_basis
):
    scale = 1.0 - decay_factor
    g, left, right = gradient[0], left_basis[0], right_basis[0]
    d, m = lax.axis_index("dp"), lax.axis_index("mp")
    at = jnp.stack([d >> 1, m >> 1, m & 1, d & 1]).astype(jnp.int32)

    both = lax.all_gather(
        jnp.stack([left, g]), "dp", axis=1, axis_index_groups=Z_GROUPS, tiled=True
    )
    both = both.reshape(2, N, SIDE, SIDE)
    r_block = to_swapped(right, 0)
    g_own = from_plane(g)
    g_own = pack(at, g_own)
    r_own = exchange_plane(jnp.broadcast_to(r_block, (N, SIDE, SIDE)))
    g_other = other_core(g_own)
    r_other = other_core(r_own)
    g_beside = neighbour(g)

    keep, send = contract(at, both, g_own, g_other, TN, 0)
    turned = neighbour(send)
    rotated_left = (keep + turned.astype(f32)).astype(bf16)
    rotated_left = exchange_z(jnp.broadcast_to(rotated_left, (N, SIDE, SIDE)))
    keep, send = contract(at, rotated_left, r_own, r_other, NN)
    terms = spread(at, g, g_beside, g_own, g_other)
    terms = lax.optimization_barrier((terms, keep))[0].reshape(N * SIDE, SIDE)
    left_sum = lax.psum_scatter(terms, "dp", axis_index_groups=Z_GROUPS, tiled=True)
    new_left = decay_factor * left_factor[0] + scale * left_sum.astype(f32)
    turned = neighbour(send)
    rotated = keep + turned.astype(f32)

    new_first = decay_moment * first_moment[0] + (1.0 - decay_moment) * rotated
    new_second = decay_moment * second_moment[0] + (1.0 - decay_moment) * rotated * rotated
    direction = (new_first / (jnp.sqrt(new_second) + epsilon)).astype(bf16)

    left_panel = both[0]
    first = placed(left_panel, swap)
    second = placed(left_panel, lambda d, m: swap(d, m ^ 1))
    direction_beside = other_core(direction)
    terms = rotate_back(at, first, second, direction, direction_beside)
    terms = exchange_plane(terms)
    back_left = jnp.sum(terms, axis=0, dtype=f32).astype(bf16)
    back_beside = neighbour(back_left)
    keep, *terms = spread_apart(at, back_left, back_beside, r_own, r_other)
    updates = [along_z(terms[s - 1], s) for s in (4, 3, 5, 2, 6, 1, 7)]
    mine, theirs = right_terms(at, both, g, g_beside)
    theirs = other_core(theirs)
    sends = chip_sum(at, mine, theirs)
    arrived = [to_swapped(sends[t], t) for t in (6, 5, 7, 2)]
    arrived += [to_swapped(sends[t], t) for t in (4, 1, 3, 0)]
    right_sum = sum(a.astype(f32) for a in arrived)
    new_right = decay_factor * right_factor[0] + scale * right_sum
    keep, new_left, new_right = lax.optimization_barrier((keep, new_left, new_right))
    update = (keep + sum(a.astype(f32) for a in updates)).astype(bf16)
    return tuple(x[None] for x in (new_first, new_second, new_left, new_right, update))


def solution(mesh):
    in_specs = (P(None, "mp", "dp"),) * 5 + (P(None, "dp", "mp"), P(None, "mp", "dp"))
    out_specs = (P(None, "mp", "dp"),) * 5
    return jax.shard_map(
        update_step, mesh=mesh, in_specs=in_specs, out_specs=out_specs, check_vma=False
    )
```
